32 devices in a mesh: batch: 1 (over z), seq_hi: 4 (over y), seq: 8 (over x, core).
Axes of the slice: x: 4, y: 4, z: 1, core: 2. Of those that a mesh axis runs over, the one named last changes fastest.
The devices are a block of a 4x4x8 slice.
Arguments:
- x_seq: bfloat16 [32, 1024, 512], P('batch', ('seq_hi', 'seq'))
- w_f0: bfloat16 [3, 10, 512, 512], replicated
- w_f1: bfloat16 [3, 10, 512, 512], replicated
- w_g0: bfloat16 [3, 10, 512, 512], replicated
- w_g1: bfloat16 [3, 10, 512, 512], replicated
- w_res: bfloat16 [3, 10, 512, 512], replicated
- w_skip: bfloat16 [3, 10, 512, 256], replicated
Outputs:
- output 1: float32 [32, 1024, 512], P('batch', ('seq_hi', 'seq'))
- output 2: float32 [32, 1024, 256], P('batch', ('seq_hi', 'seq'))
All inputs are finite; a program needn't handle non-finite values.
Results may differ from the reference program's by a relative error of at most 0.00955824.
Values are sent between devices in bfloat16 or wider.
A program may use at most 768 MiB of HBM per device.

```python
import jax
import jax.numpy as jnp
from jax import lax

GROUP_SEQS = 32
SEQ_LEN = 1024
CHANNELS = 512
SKIP_CH = 256
DIL_CYCLE = 10
REPEATS = 3


def setup_inputs(seed: int = 0, part: int = 0) -> dict:
    keys = jax.random.split(jax.random.key(seed), 7)
    square = (REPEATS, DIL_CYCLE, CHANNELS, CHANNELS)
    tap_scale = (2 * CHANNELS) ** -0.5
    x_seq = jax.random.normal(jax.random.fold_in(keys[0], part), (GROUP_SEQS, SEQ_LEN, CHANNELS), jnp.float32)
    w_f0 = jax.random.normal(keys[1], square, jnp.float32) * tap_scale
    w_f1 = jax.random.normal(keys[2], square, jnp.float32) * tap_scale
    w_g0 = jax.random.normal(keys[3], square, jnp.float32) * tap_scale
    w_g1 = jax.random.normal(keys[4], square, jnp.float32) * tap_scale
    w_res = jax.random.normal(keys[5], square, jnp.float32) * (0.5 * CHANNELS ** -0.5)
    w_skip = jax.random.normal(keys[6], (REPEATS, DIL_CYCLE, CHANNELS, SKIP_CH), jnp.float32) * CHANNELS ** -0.5
    return {
        "x_seq": x_seq.astype(jnp.bfloat16),
        "w_f0": w_f0.astype(jnp.bfloat16),
        "w_f1": w_f1.astype(jnp.bfloat16),
        "w_g0": w_g0.astype(jnp.bfloat16),
        "w_g1": w_g1.astype(jnp.bfloat16),
        "w_res": w_res.astype(jnp.bfloat16),
        "w_skip": w_skip.astype(jnp.bfloat16),
    }


def mat_mul(left, right):
    return jnp.dot(left, right, preferred_element_type=jnp.float32)


def reference(x_seq, w_f0, w_f1, w_g0, w_g1, w_res, w_skip):
    def one_sequence(seq_in):
        residual = seq_in.astype(jnp.float32)
        skip_acc = jnp.zeros((SEQ_LEN, SKIP_CH), jnp.float32)
        for rep_idx in range(REPEATS):
            for cyc_idx in range(DIL_CYCLE):
                dilation = 2 ** cyc_idx
                current = residual.astype(jnp.bfloat16)
                delayed = jnp.pad(current[:SEQ_LEN - dilation], ((dilation, 0), (0, 0)))
                filter_pre = mat_mul(current, w_f1[rep_idx, cyc_idx]) + mat_mul(delayed, w_f0[rep_idx, cyc_idx])
                gate_pre = mat_mul(current, w_g1[rep_idx, cyc_idx]) + mat_mul(delayed, w_g0[rep_idx, cyc_idx])
                activated = (jnp.tanh(filter_pre) * jax.nn.sigmoid(gate_pre)).astype(jnp.bfloat16)
                residual = residual + mat_mul(activated, w_res[rep_idx, cyc_idx])
                skip_acc = skip_acc + mat_mul(activated, w_skip[rep_idx, cyc_idx])
        return residual, skip_acc
    h_out, skip_out = lax.map(one_sequence, x_seq)
    return h_out, skip_out
```

```python
import functools

import jax
import jax.numpy as jnp
from jax import lax
from jax.experimental import pallas as pl
from jax.experimental.pallas import tpu as pltpu
from jax.sharding import PartitionSpec as P

SEQ_AXES = ("seq_hi", "seq")
MESH = pl.DeviceIdType.MESH

TEAM = 2
ROW_TILE = 256
COL_TILE = 256
ALIGN = 16
N_BUF = 5
AHEAD = N_BUF - 1


def halo_layout(n_cyc):
    sizes = [max(2 ** cyc, ALIGN) for cyc in range(n_cyc)]
    starts = [sum(sizes[:cyc]) for cyc in range(n_cyc)]
    return starts, sizes, sum(sizes)


def stack_kernel(n_hi, n_lo, n_rep, n_cyc, x_ref, wf0_ref, wf1_ref, wg0_ref, wg1_ref, wr_ref, ws_ref, h_out, skip_out,
                 x_buf, h_acc, skip_acc, u_buf, halo, w_sq, w_sk,
                 w_sem, x_send, x_recv, halo_send, halo_recv, h_send, h_recv, s_send, s_recv):
    n_dev = n_hi * n_lo
    block_len, chans = x_ref.shape[1], x_ref.shape[2]
    skip_ch = skip_out.shape[2]
    part_rows = h_acc.shape[1]
    per_part = n_dev // TEAM
    half_starts, halo_sizes, _ = halo_layout(n_cyc)
    n_layers = n_rep * n_cyc

    group = lax.axis_index("batch")
    me = lax.axis_index("seq_hi") * n_lo + lax.axis_index("seq")
    team = me // TEAM
    part = me % TEAM

    def device(index):
        return (group, index // n_lo, index % n_lo)

    squares = (wf0_ref, wf1_ref, wg0_ref, wg1_ref, wr_ref)

    def weight_copies(rep, cyc):
        slot = cyc % N_BUF
        copies = [pltpu.make_async_copy(ref.at[rep, cyc], w_sq.at[slot, i], w_sem.at[slot, i]) for i, ref in enumerate(squares)]
        copies.append(pltpu.make_async_copy(ws_ref.at[rep, cyc], w_sk.at[slot], w_sem.at[slot, len(squares)]))
        return copies

    for cyc in range(AHEAD):
        for copy in weight_copies(0, cyc):
            copy.start()

    barrier = pltpu.get_barrier_semaphore()

    def greet(index, _):
        @pl.when(index != me)
        def _():
            pl.semaphore_signal(barrier, inc=1, device_id=device(index), device_id_type=MESH)
        return 0

    lax.fori_loop(0, n_dev, greet, 0)
    pl.semaphore_wait(barrier, n_dev - 1)

    def x_target(step):
        to_team = (team + step) % per_part
        return to_team, to_team * TEAM + me // per_part

    def x_copies(seq, to_team, target, remote):
        src = x_ref.at[to_team * TEAM + seq]
        place = me % per_part
        dst = x_buf.at[seq, pl.ds(place * block_len, block_len)]
        if remote:
            return pltpu.make_async_remote_copy(src_ref=src, dst_ref=dst, send_sem=x_send.at[seq, to_team], recv_sem=x_recv.at[seq, place],
                                                device_id=device(target), device_id_type=MESH)
        return pltpu.make_async_copy(src, dst, x_recv.at[seq, place])

    for seq in range(TEAM):
        def send_x(step, _, seq=seq):
            to_team, target = x_target(step)

            @pl.when(target != me)
            def _():
                x_copies(seq, to_team, target, True).start()

            @pl.when(target == me)
            def _():
                x_copies(seq, to_team, target, False).start()
            return 0

        lax.fori_loop(0, per_part, send_x, 0)

    zero_slot = TEAM * n_rep
    halo[zero_slot] = jnp.zeros(halo.shape[1:], halo.dtype)

    def halo_copy(slot, cyc):
        size = halo_sizes[cyc]
        return pltpu.make_async_remote_copy(
            src_ref=u_buf.at[cyc % 2, pl.ds(part_rows - size, size)],
            dst_ref=halo.at[slot, pl.ds(half_starts[cyc], size)],
            send_sem=halo_send.at[cyc % 2],
            recv_sem=halo_recv.at[slot, cyc],
            device_id=device(team * TEAM + (TEAM - 1)),
            device_id_type=MESH,
        )

    n_tiles = part_rows // ROW_TILE

    def delayed_tile(cyc, tile, read_slot):
        dil = 2 ** cyc
        first = tile * ROW_TILE
        start = half_starts[cyc]
        cur = u_buf.at[cyc % 2]
        if dil % ALIGN == 0:
            if first + ROW_TILE <= dil:
                return halo[read_slot, pl.ds(start + first, ROW_TILE), :]
            if first >= dil:
                return cur[pl.ds(first - dil, ROW_TILE), :]
            return jnp.concatenate([halo[read_slot, pl.ds(start + first, dil - first), :], cur[pl.ds(0, ROW_TILE - dil + first), :]], axis=0)
        if first == 0:
            before = halo[read_slot, pl.ds(start, ALIGN), :]
        else:
            before = cur[pl.ds(first - ALIGN, ALIGN), :]
        both = jnp.concatenate([before, cur[pl.ds(first, ROW_TILE), :]], axis=0).astype(jnp.float32)
        return pltpu.roll(both, dil, 0)[ALIGN:].astype(jnp.bfloat16)

    def dot(left, right):
        return jnp.dot(left, right, preferred_element_type=jnp.float32)

    def layer(seq, rep, cyc):
        wslot = cyc % N_BUF
        slot = seq * n_rep + rep
        read_slot = jnp.where(part == 0, zero_slot, slot)

        for copy in weight_copies(rep, cyc):
            copy.wait()
        nxt_cyc = (cyc + AHEAD) % n_cyc
        nxt_rep = rep + (cyc + AHEAD) // n_cyc

        @pl.when(jnp.logical_or(nxt_rep < n_rep, seq + 1 < TEAM))
        def _():
            for copy in weight_copies(nxt_rep % n_rep, nxt_cyc):
                copy.start()

        @pl.when(part == 0)
        def _():
            halo_copy(slot, cyc).start()

        @pl.when(part == TEAM - 1)
        def _():
            halo_copy(slot, cyc).wait_recv()

        cur, nxt = u_buf.at[cyc % 2], u_buf.at[(cyc + 1) % 2]
        acts = []
        for tile in range(n_tiles):
            rows = pl.ds(tile * ROW_TILE, ROW_TILE)
            now = cur[rows, :]
            before = delayed_tile(cyc, tile, read_slot)
            pieces = []
            for col in range(0, chans, COL_TILE):
                cols = pl.ds(col, COL_TILE)
                f = dot(now, w_sq[wslot, 1, :, cols]) + dot(before, w_sq[wslot, 0, :, cols])
                g = dot(now, w_sq[wslot, 3, :, cols]) + dot(before, w_sq[wslot, 2, :, cols])
                pieces.append((jnp.tanh(f) * (0.5 * jnp.tanh(0.5 * g) + 0.5)).astype(jnp.bfloat16))
            acts.append(jnp.concatenate(pieces, axis=1))
        for tile in range(n_tiles):
            rows = pl.ds(tile * ROW_TILE, ROW_TILE)
            for col in range(0, chans, COL_TILE):
                cols = pl.ds(col, COL_TILE)
                new = h_acc[seq, rows, cols] + dot(acts[tile], w_sq[wslot, 4, :, cols])
                h_acc[seq, rows, cols] = new
                nxt[rows, cols] = new.astype(jnp.bfloat16)
            skip_acc[seq, rows, :] += dot(acts[tile], w_sk[wslot])

        @pl.when(part == 0)
        def _():
            halo_copy(slot, cyc).wait_send()

    def out_copies(seq, step, remote):
        place = (me + step) % per_part
        target = part * per_part + place
        rows = pl.ds(place * block_len, block_len)
        which = team * TEAM + seq
        pairs = ((h_acc, h_out, h_send, h_recv), (skip_acc, skip_out, s_send, s_recv))
        if remote:
            return target, [pltpu.make_async_remote_copy(src_ref=acc.at[seq, rows], dst_ref=out.at[which], send_sem=send.at[seq, place],
                                                         recv_sem=recv.at[seq, team], device_id=device(target), device_id_type=MESH)
                            for acc, out, send, recv in pairs]
        return target, [pltpu.make_async_copy(acc.at[seq, rows], out.at[which], recv.at[seq, team]) for acc, out, send, recv in pairs]

    def one_sequence(seq, _):
        def wait_x(place, _):
            dst = x_buf.at[seq, pl.ds(place * block_len, block_len)]
            pltpu.make_async_copy(dst, dst, x_recv.at[seq, place]).wait()
            return 0

        lax.fori_loop(0, per_part, wait_x, 0)
        start = x_buf[seq]
        u_buf[0] = start
        h_acc[seq] = start.astype(jnp.float32)
        skip_acc[seq] = jnp.zeros(skip_acc.shape[1:], jnp.float32)

        def one_cycle(rep, _):
            for cyc in range(n_cyc):
                layer(seq, rep, cyc)
            return 0

        lax.fori_loop(0, n_rep, one_cycle, 0)

        def send_out(step, _):
            target, copies = out_copies(seq, step, True)

            @pl.when(target != me)
            def _():
                for copy in copies:
                    copy.start()

            @pl.when(target == me)
            def _():
                for copy in out_copies(seq, step, False)[1]:
                    copy.start()
            return 0

        lax.fori_loop(0, per_part, send_out, 0)
        return 0

    lax.fori_loop(0, TEAM, one_sequence, 0)

    for seq in range(TEAM):
        def finish(step, _, seq=seq):
            to_team, target = x_target(step)

            @pl.when(target != me)
            def _():
                x_copies(seq, to_team, target, True).wait_send()
            target, copies = out_copies(seq, step, True)

            @pl.when(target != me)
            def _():
                for copy in copies:
                    copy.wait_send()
            dst = h_out.at[step * TEAM + seq]
            pltpu.make_async_copy(dst, dst, h_recv.at[seq, step]).wait()
            dst = skip_out.at[step * TEAM + seq]
            pltpu.make_async_copy(dst, dst, s_recv.at[seq, step]).wait()
            return 0

        lax.fori_loop(0, per_part, finish, 0)


def solution(mesh):
    n_hi, n_lo = mesh.shape["seq_hi"], mesh.shape["seq"]
    n_dev = n_hi * n_lo
    seq_spec = P("batch", SEQ_AXES, None)

    def local_stack(x_loc, w_f0, w_f1, w_g0, w_g1, w_res, w_skip):
        n_seq, block_len, chans = x_loc.shape
        n_rep, n_cyc, skip_ch = w_f0.shape[0], w_f0.shape[1], w_skip.shape[-1]
        assert n_seq == n_dev and n_dev % TEAM == 0 and n_cyc % N_BUF == 0 and n_cyc % 2 == 0
        part_rows = n_dev * block_len // TEAM
        per_part = n_dev // TEAM
        assert part_rows >= 2 ** (n_cyc - 1) and part_rows % ROW_TILE == 0
        halo_rows = halo_layout(n_cyc)[2]
        sem = pltpu.SemaphoreType.DMA
        return pl.pallas_call(
            functools.partial(stack_kernel, n_hi, n_lo, n_rep, n_cyc),
            out_shape=(jax.ShapeDtypeStruct((n_seq, block_len, chans), jnp.float32),
                       jax.ShapeDtypeStruct((n_seq, block_len, skip_ch), jnp.float32)),
            in_specs=[pl.BlockSpec(memory_space=pl.ANY)] * 7,
            out_specs=(pl.BlockSpec(memory_space=pl.ANY),) * 2,
            scratch_shapes=[
                pltpu.VMEM((TEAM, part_rows, chans), jnp.bfloat16),
                pltpu.VMEM((TEAM, part_rows, chans), jnp.float32),
                pltpu.VMEM((TEAM, part_rows, skip_ch), jnp.float32),
                pltpu.VMEM((2, part_rows, chans), jnp.bfloat16),
                pltpu.VMEM((TEAM * n_rep + 1, halo_rows, chans), jnp.bfloat16),
                pltpu.VMEM((N_BUF, 5, chans, chans), jnp.bfloat16),
                pltpu.VMEM((N_BUF, chans, skip_ch), jnp.bfloat16),
                sem((N_BUF, 6)),
                sem((TEAM, per_part)),
                sem((TEAM, per_part)),
                sem((2,)),
                sem((TEAM * n_rep, n_cyc)),
                sem((TEAM, per_part)),
                sem((TEAM, per_part)),
                sem((TEAM, per_part)),
                sem((TEAM, per_part)),
            ],
            compiler_params=pltpu.CompilerParams(collective_id=0, has_side_effects=True, vmem_limit_bytes=60 * 1024 * 1024),
        )(x_loc, w_f0, w_f1, w_g0, w_g1, w_res, w_skip)

    return jax.shard_map(local_stack, mesh=mesh, in_specs=(seq_spec, P(), P(), P(), P(), P(), P()), out_specs=(seq_spec, seq_spec), check_vma=False)
```

```python
import functools

import jax
import jax.numpy as jnp
from jax import lax
from jax.experimental import pallas as pl
from jax.experimental.pallas import tpu as pltpu
from jax.sharding import PartitionSpec as P

SEQ_AXES = ("seq_hi", "seq")
MESH = pl.DeviceIdType.MESH

TEAM = 2
ROW_TILE = 256
COL_TILE = 256
ALIGN = 16
GROUP = 2
U_BUF = 5
FIRST = 4


def halo_layout(n_cyc):
    sizes = [max(2 ** cyc, ALIGN) for cyc in range(n_cyc)]
    starts = [sum(sizes[:cyc]) for cyc in range(n_cyc)]
    return starts, sizes, sum(sizes)


def stack_kernel(n_hi, n_lo, n_rep, n_cyc, x_ref, wf0_ref, wf1_ref, wg0_ref, wg1_ref, wr_ref, ws_ref, h_out, skip_out,
                 x_buf, h_acc, skip_acc, u_buf, halo, w_sq, w_sk,
                 w_sem, x_send, x_recv, halo_send, halo_recv, h_send, h_recv, s_send, s_recv):
    n_dev = n_hi * n_lo
    block_len, chans = x_ref.shape[1], x_ref.shape[2]
    skip_ch = skip_out.shape[2]
    part_rows = h_acc.shape[1]
    per_part = n_dev // TEAM
    half_starts, halo_sizes, _ = halo_layout(n_cyc)
    n_layers = n_rep * n_cyc

    group = lax.axis_index("batch")
    me = lax.axis_index("seq_hi") * n_lo + lax.axis_index("seq")
    team = me // TEAM
    part = me % TEAM

    def device(index):
        return (group, index // n_lo, index % n_lo)

    squares = (wf0_ref, wf1_ref, wg0_ref, wg1_ref, wr_ref)

    def weight_copies(rep, cyc):
        slot = cyc
        copies = [pltpu.make_async_copy(ref.at[rep, cyc], w_sq.at[slot, i], w_sem.at[slot, i]) for i, ref in enumerate(squares)]
        copies.append(pltpu.make_async_copy(ws_ref.at[rep, cyc], w_sk.at[slot], w_sem.at[slot, len(squares)]))
        return copies

    def first_weights(start, end):
        for cyc in range(start, end):
            for copy in weight_copies(0, cyc):
                copy.start()

    first_weights(0, FIRST)

    barrier = pltpu.get_barrier_semaphore()

    def greet(index, _):
        @pl.when(index != me)
        def _():
            pl.semaphore_signal(barrier, inc=1, device_id=device(index), device_id_type=MESH)
        return 0

    lax.fori_loop(0, n_dev, greet, 0)
    pl.semaphore_wait(barrier, n_dev - 1)

    def x_target(step):
        to_team = (team + step) % per_part
        return to_team, to_team * TEAM + me // per_part

    def x_copies(seq, to_team, target, remote):
        src = x_ref.at[to_team * TEAM + seq]
        place = me % per_part
        dst = x_buf.at[seq, pl.ds(place * block_len, block_len)]
        if remote:
            return pltpu.make_async_remote_copy(src_ref=src, dst_ref=dst, send_sem=x_send.at[seq, to_team], recv_sem=x_recv.at[seq, place],
                                                device_id=device(target), device_id_type=MESH)
        return pltpu.make_async_copy(src, dst, x_recv.at[seq, place])

    def send_all_x(seq):
        def send_x(step, _):
            to_team, target = x_target(step)

            @pl.when(target != me)
            def _():
                x_copies(seq, to_team, target, True).start()

            @pl.when(target == me)
            def _():
                x_copies(seq, to_team, target, False).start()
            return 0

        lax.fori_loop(0, per_part, send_x, 0)

    send_all_x(0)
    first_weights(FIRST, n_cyc - GROUP)
    zero_slot = TEAM * n_rep
    halo[zero_slot] = jnp.zeros(halo.shape[1:], halo.dtype)

    def halo_copy(slot, cyc):
        size = halo_sizes[cyc]
        return pltpu.make_async_remote_copy(
            src_ref=u_buf.at[cyc % U_BUF, pl.ds(part_rows - size, size)],
            dst_ref=halo.at[slot, pl.ds(half_starts[cyc], size)],
            send_sem=halo_send.at[cyc],
            recv_sem=halo_recv.at[slot, cyc],
            device_id=device(team * TEAM + (TEAM - 1)),
            device_id_type=MESH,
        )

    n_tiles = part_rows // ROW_TILE

    def delayed_tile(cyc, tile, read_slot):
        dil = 2 ** cyc
        first = tile * ROW_TILE
        start = half_starts[cyc]
        cur = u_buf.at[cyc % U_BUF]
        if dil % ALIGN == 0:
            if first + ROW_TILE <= dil:
                return halo[read_slot, pl.ds(start + first, ROW_TILE), :]
            if first >= dil:
                return cur[pl.ds(first - dil, ROW_TILE), :]
            return jnp.concatenate([halo[read_slot, pl.ds(start + first, dil - first), :], cur[pl.ds(0, ROW_TILE - dil + first), :]], axis=0)
        if first == 0:
            before = halo[read_slot, pl.ds(start, ALIGN), :]
        else:
            before = cur[pl.ds(first - ALIGN, ALIGN), :]
        both = jnp.concatenate([before, cur[pl.ds(first, ROW_TILE), :]], axis=0).astype(jnp.float32)
        return pltpu.roll(both, dil, 0)[ALIGN:].astype(jnp.bfloat16)

    def dot(left, right):
        return jnp.dot(left, right, preferred_element_type=jnp.float32)

    def sent_at(first):
        return range(max(first - GROUP + 1, 0), min(first + 1, n_cyc))

    def stop(seq, rep, first):
        slot = seq * n_rep + rep

        def weights(cyc, act):
            at_rep = rep + cyc // n_cyc
            copies = weight_copies(at_rep % n_rep, cyc % n_cyc)
            if cyc < n_cyc:
                for copy in copies:
                    act(copy)
            else:
                @pl.when(jnp.logical_or(at_rep < n_rep, seq + 1 < TEAM))
                def _():
                    for copy in copies:
                        act(copy)

        @pl.when(part == 0)
        def _():
            for cyc in sent_at(first):
                halo_copy(slot, cyc).start()

        for cyc in range(first + n_cyc - GROUP, first + n_cyc):
            weights(cyc, lambda copy: copy.start())

        if first < n_cyc:
            before = first - GROUP
            gone = list(sent_at(before)) if before >= 0 else []
            gone_prev = list(sent_at(before + n_cyc)) if before < 0 else list(sent_at(n_cyc)) if before == 0 else []

            @pl.when(part == 0)
            def _():
                for cyc in gone:
                    halo_copy(slot, cyc).wait_send()

            @pl.when(jnp.logical_and(part == 0, slot > 0))
            def _():
                for cyc in gone_prev:
                    halo_copy(slot, cyc).wait_send()

            for cyc in range(first + GROUP, first + 2 * GROUP):
                weights(cyc, lambda copy: copy.wait())

            @pl.when(part == TEAM - 1)
            def _():
                for cyc in range(first, first + GROUP):
                    halo_copy(slot, cyc).wait_recv()

    def cycle_end(seq, rep):
        if GROUP > 1:
            @pl.when(part == 0)
            def _():
                for cyc in range(n_cyc - GROUP + 1, n_cyc):
                    halo_copy(seq * n_rep + rep, cyc).start()


    def layer(seq, rep, cyc):
        slot = seq * n_rep + rep
        read_slot = jnp.where(part == 0, zero_slot, slot)
        cur, nxt = u_buf.at[cyc % U_BUF], u_buf.at[(cyc + 1) % U_BUF]
        acts = []
        for tile in range(n_tiles):
            rows = pl.ds(tile * ROW_TILE, ROW_TILE)
            now = cur[rows, :]
            before = delayed_tile(cyc, tile, read_slot)
            pieces = []
            for col in range(0, chans, COL_TILE):
                cols = pl.ds(col, COL_TILE)
                f = dot(now, w_sq[cyc, 1, :, cols]) + dot(before, w_sq[cyc, 0, :, cols])
                g = dot(now, w_sq[cyc, 3, :, cols]) + dot(before, w_sq[cyc, 2, :, cols])
                pieces.append((jnp.tanh(f) * (0.5 * jnp.tanh(0.5 * g) + 0.5)).astype(jnp.bfloat16))
            acts.append(jnp.concatenate(pieces, axis=1))
        for tile in range(n_tiles):
            rows = pl.ds(tile * ROW_TILE, ROW_TILE)
            for col in range(0, chans, COL_TILE):
                cols = pl.ds(col, COL_TILE)
                new = h_acc[seq, rows, cols] + dot(acts[tile], w_sq[cyc, 4, :, cols])
                h_acc[seq, rows, cols] = new
                nxt[rows, cols] = new.astype(jnp.bfloat16)
            skip_acc[seq, rows, :] += dot(acts[tile], w_sk[cyc])

    def out_copies(seq, step, remote):
        place = (2 * ((me // 2 + step) % (per_part // 2)) + step // (per_part // 2)) % per_part
        target = part * per_part + place
        rows = pl.ds(place * block_len, block_len)
        which = team * TEAM + seq
        pairs = ((h_acc, h_out, h_send, h_recv), (skip_acc, skip_out, s_send, s_recv))
        if remote:
            return target, [pltpu.make_async_remote_copy(src_ref=acc.at[seq, rows], dst_ref=out.at[which], send_sem=send.at[seq, place],
                                                         recv_sem=recv.at[seq, team], device_id=device(target), device_id_type=MESH)
                            for acc, out, send, recv in pairs]
        return target, [pltpu.make_async_copy(acc.at[seq, rows], out.at[which], recv.at[seq, team]) for acc, out, send, recv in pairs]

    def wait_x(seq, place, _):
        dst = x_buf.at[seq, pl.ds(place * block_len, block_len)]
        pltpu.make_async_copy(dst, dst, x_recv.at[seq, place]).wait()
        return 0

    early = per_part // 2
    lax.fori_loop(0, early, functools.partial(wait_x, 0), 0)
    for seq in range(1, TEAM):
        send_all_x(seq)

    def one_sequence(seq, _):
        lax.fori_loop(jnp.where(seq == 0, early, 0), per_part, functools.partial(wait_x, seq), 0)
        start = x_buf[seq]
        u_buf[0] = start
        h_acc[seq] = start.astype(jnp.float32)
        skip_acc[seq] = jnp.zeros(skip_acc.shape[1:], jnp.float32)

        def one_cycle(rep, _):
            for first in range(0, n_cyc, GROUP):
                stop(seq, rep, first)
                for cyc in range(first, first + GROUP):
                    layer(seq, rep, cyc)
            cycle_end(seq, rep)
            return 0

        lax.fori_loop(0, n_rep, one_cycle, 0)

        def send_out(step, _):
            target, copies = out_copies(seq, step, True)

            @pl.when(target != me)
            def _():
                for copy in copies:
                    copy.start()

            @pl.when(target == me)
            def _():
                for copy in out_copies(seq, step, False)[1]:
                    copy.start()
            return 0

        lax.fori_loop(0, per_part, send_out, 0)
        return 0

    for cyc in range(GROUP):
        for copy in weight_copies(0, cyc):
            copy.wait()
    lax.fori_loop(0, TEAM, one_sequence, 0)

    @pl.when(part == 0)
    def _():
        for cyc in range(n_cyc - 2 * GROUP + 1, n_cyc):
            halo_copy(0, cyc).wait_send()

    for seq in range(TEAM):
        def finish(step, _, seq=seq):
            to_team, target = x_target(step)

            @pl.when(target != me)
            def _():
                x_copies(seq, to_team, target, True).wait_send()
            target, copies = out_copies(seq, step, True)

            @pl.when(target != me)
            def _():
                for copy in copies:
                    copy.wait_send()
            dst = h_out.at[step * TEAM + seq]
            pltpu.make_async_copy(dst, dst, h_recv.at[seq, step]).wait()
            dst = skip_out.at[step * TEAM + seq]
            pltpu.make_async_copy(dst, dst, s_recv.at[seq, step]).wait()
            return 0

        lax.fori_loop(0, per_part, finish, 0)


def solution(mesh):
    n_hi, n_lo = mesh.shape["seq_hi"], mesh.shape["seq"]
    n_dev = n_hi * n_lo
    seq_spec = P("batch", SEQ_AXES, None)

    def local_stack(x_loc, w_f0, w_f1, w_g0, w_g1, w_res, w_skip):
        n_seq, block_len, chans = x_loc.shape
        n_rep, n_cyc, skip_ch = w_f0.shape[0], w_f0.shape[1], w_skip.shape[-1]
        assert n_seq == n_dev and n_dev % TEAM == 0 and n_cyc % GROUP == 0 and n_cyc % U_BUF == 0
        part_rows = n_dev * block_len // TEAM
        per_part = n_dev // TEAM
        assert part_rows >= 2 ** (n_cyc - 1) and part_rows % ROW_TILE == 0
        halo_rows = halo_layout(n_cyc)[2]
        sem = pltpu.SemaphoreType.DMA
        return pl.pallas_call(
            functools.partial(stack_kernel, n_hi, n_lo, n_rep, n_cyc),
            out_shape=(pltpu.VMEM((n_seq, block_len, chans), jnp.float32), pltpu.VMEM((n_seq, block_len, skip_ch), jnp.float32)),
            in_specs=[pl.BlockSpec(memory_space=pl.ANY)] * 7,
            out_specs=(pl.BlockSpec(memory_space=pltpu.VMEM),) * 2,
            scratch_shapes=[
                pltpu.VMEM((TEAM, part_rows, chans), jnp.bfloat16),
                pltpu.VMEM((TEAM, part_rows, chans), jnp.float32),
                pltpu.VMEM((TEAM, part_rows, skip_ch), jnp.float32),
                pltpu.VMEM((U_BUF, part_rows, chans), jnp.bfloat16),
                pltpu.VMEM((TEAM * n_rep + 1, halo_rows, chans), jnp.bfloat16),
                pltpu.VMEM((n_cyc, 5, chans, chans), jnp.bfloat16),
                pltpu.VMEM((n_cyc, chans, skip_ch), jnp.bfloat16),
                sem((n_cyc, 6)),
                sem((TEAM, per_part)),
                sem((TEAM, per_part)),
                sem((n_cyc,)),
                sem((TEAM * n_rep, n_cyc)),
                sem((TEAM, per_part)),
                sem((TEAM, per_part)),
                sem((TEAM, per_part)),
                sem((TEAM, per_part)),
            ],
            compiler_params=pltpu.CompilerParams(collective_id=0, has_side_effects=True, vmem_limit_bytes=52 * 1024 * 1024),
        )(x_loc, w_f0, w_f1, w_g0, w_g1, w_res, w_skip)

    return jax.shard_map(local_stack, mesh=mesh, in_specs=(seq_spec, P(), P(), P(), P(), P(), P()), out_specs=(seq_spec, seq_spec), check_vma=False)
```

```python
import functools

import jax
import jax.numpy as jnp
from jax import lax
from jax.experimental import pallas as pl
from jax.experimental.pallas import tpu as pltpu
from jax.sharding import PartitionSpec as P

SEQ_AXES = ("seq_hi", "seq")
MESH = pl.DeviceIdType.MESH

TEAM = 2
ROW_TILE = 256
COL_TILE = 256
ALIGN = 16
GROUP = 2
U_BUF = 5
FIRST = 2


def halo_layout(n_cyc):
    sizes = [max(2 ** cyc, ALIGN) for cyc in range(n_cyc)]
    starts = [sum(sizes[:cyc]) for cyc in range(n_cyc)]
    return starts, sizes, sum(sizes)


def stack_kernel(n_hi, n_lo, n_rep, n_cyc, x_ref, wf0_ref, wf1_ref, wg0_ref, wg1_ref, wr_ref, ws_ref, h_out, skip_out,
                 x_buf, h_acc, skip_acc, u_buf, halo, w_sq, w_sk,
                 w_sem, x_send, x_recv, halo_send, halo_recv, h_send, h_recv, s_send, s_recv):
    n_dev = n_hi * n_lo
    block_len, chans = x_ref.shape[1], x_ref.shape[2]
    skip_ch = skip_out.shape[2]
    part_rows = h_acc.shape[1]
    per_part = n_dev // TEAM
    half_starts, halo_sizes, _ = halo_layout(n_cyc)
    n_layers = n_rep * n_cyc

    group = lax.axis_index("batch")
    me = lax.axis_index("seq_hi") * n_lo + lax.axis_index("seq")
    team = me // TEAM
    part = me % TEAM

    def device(index):
        return (group, index // n_lo, index % n_lo)

    squares = (wf0_ref, wf1_ref, wg0_ref, wg1_ref, wr_ref)

    def weight_copies(rep, cyc):
        slot = cyc
        copies = [pltpu.make_async_copy(ref.at[rep, cyc], w_sq.at[slot, i], w_sem.at[slot, 0]) for i, ref in enumerate(squares)]
        copies.append(pltpu.make_async_copy(ws_ref.at[rep, cyc], w_sk.at[slot], w_sem.at[slot, 1]))
        return copies

    def weight_waits(cyc):
        return [pltpu.make_async_copy(buf.at[cyc], buf.at[cyc], w_sem.at[cyc, i]) for i, buf in enumerate((w_sq, w_sk))]

    def first_weights(start, end):
        for cyc in range(start, end):
            for copy in weight_copies(0, cyc):
                copy.start()

    first_weights(0, FIRST)

    barrier = pltpu.get_barrier_semaphore()

    def greet(index, _):
        @pl.when(index != me)
        def _():
            pl.semaphore_signal(barrier, inc=1, device_id=device(index), device_id_type=MESH)
        return 0

    lax.fori_loop(0, n_dev, greet, 0)
    pl.semaphore_wait(barrier, n_dev - 1)

    def x_target(step):
        to_team = (team + step) % per_part
        return to_team, to_team * TEAM + me // per_part

    def x_copies(seq, to_team, target, remote):
        src = x_ref.at[to_team * TEAM + seq]
        place = me % per_part
        dst = x_buf.at[seq, pl.ds(place * block_len, block_len)]
        if remote:
            return pltpu.make_async_remote_copy(src_ref=src, dst_ref=dst, send_sem=x_send.at[seq, to_team], recv_sem=x_recv.at[seq, place],
                                                device_id=device(target), device_id_type=MESH)
        return pltpu.make_async_copy(src, dst, x_recv.at[seq, place])

    def send_all_x(seq):
        def send_x(step, _):
            to_team, target = x_target(step)

            @pl.when(target != me)
            def _():
                x_copies(seq, to_team, target, True).start()

            @pl.when(target == me)
            def _():
                x_copies(seq, to_team, target, False).start()
            return 0

        lax.fori_loop(0, per_part, send_x, 0)

    send_all_x(0)
    first_weights(FIRST, n_cyc - GROUP)
    zero_slot = TEAM * n_rep
    halo[zero_slot] = jnp.zeros(halo.shape[1:], halo.dtype)

    def halo_copy(slot, cyc):
        size = halo_sizes[cyc]
        return pltpu.make_async_remote_copy(
            src_ref=u_buf.at[cyc % U_BUF, pl.ds(part_rows - size, size)],
            dst_ref=halo.at[slot, pl.ds(half_starts[cyc], size)],
            send_sem=halo_send.at[cyc],
            recv_sem=halo_recv.at[slot, cyc],
            device_id=device(team * TEAM + (TEAM - 1)),
            device_id_type=MESH,
        )

    n_tiles = part_rows // ROW_TILE

    def delayed_tile(cyc, tile, read_slot):
        dil = 2 ** cyc
        first = tile * ROW_TILE
        start = half_starts[cyc]
        cur = u_buf.at[cyc % U_BUF]
        if dil % ALIGN == 0:
            if first + ROW_TILE <= dil:
                return halo[read_slot, pl.ds(start + first, ROW_TILE), :]
            if first >= dil:
                return cur[pl.ds(first - dil, ROW_TILE), :]
            return jnp.concatenate([halo[read_slot, pl.ds(start + first, dil - first), :], cur[pl.ds(0, ROW_TILE - dil + first), :]], axis=0)
        if first == 0:
            before = halo[read_slot, pl.ds(start, ALIGN), :]
        else:
            before = cur[pl.ds(first - ALIGN, ALIGN), :]
        both = jnp.concatenate([before, cur[pl.ds(first, ROW_TILE), :]], axis=0).astype(jnp.float32)
        return pltpu.roll(both, dil, 0)[ALIGN:].astype(jnp.bfloat16)

    def dot(left, right):
        return jnp.dot(left, right, preferred_element_type=jnp.float32)

    def sent_at(first):
        return range(max(first - GROUP + 1, 0), min(first + 1, n_cyc))

    def stop(seq, rep, first):
        slot = seq * n_rep + rep

        def weights(cyc, start):
            at_rep = rep + cyc // n_cyc
            copies = weight_copies(at_rep % n_rep, cyc % n_cyc) if start else weight_waits(cyc % n_cyc)
            act = (lambda copy: copy.start()) if start else (lambda copy: copy.wait())
            if cyc < n_cyc:
                for copy in copies:
                    act(copy)
            else:
                @pl.when(jnp.logical_or(at_rep < n_rep, seq + 1 < TEAM))
                def _():
                    for copy in copies:
                        act(copy)

        @pl.when(part == 0)
        def _():
            for cyc in sent_at(first):
                halo_copy(slot, cyc).start()

        for cyc in range(first + n_cyc - GROUP, first + n_cyc):
            weights(cyc, True)

        if first < n_cyc:
            before = first - GROUP
            gone = list(sent_at(before)) if before >= 0 else []
            gone_prev = list(sent_at(before + n_cyc)) if before < 0 else list(sent_at(n_cyc)) if before == 0 else []

            @pl.when(part == 0)
            def _():
                for cyc in gone:
                    halo_copy(slot, cyc).wait_send()

            @pl.when(jnp.logical_and(part == 0, slot > 0))
            def _():
                for cyc in gone_prev:
                    halo_copy(slot, cyc).wait_send()

            for cyc in range(first + GROUP, first + 2 * GROUP):
                weights(cyc, False)

            @pl.when(part == TEAM - 1)
            def _():
                for cyc in range(first, first + GROUP):
                    halo_copy(slot, cyc).wait_recv()

    def cycle_end(seq, rep):
        if GROUP > 1:
            @pl.when(part == 0)
            def _():
                for cyc in range(n_cyc - GROUP + 1, n_cyc):
                    halo_copy(seq * n_rep + rep, cyc).start()


    def layer(seq, rep, cyc):
        slot = seq * n_rep + rep
        read_slot = jnp.where(part == 0, zero_slot, slot)
        cur, nxt = u_buf.at[cyc % U_BUF], u_buf.at[(cyc + 1) % U_BUF]
        acts = []
        for tile in range(n_tiles):
            rows = pl.ds(tile * ROW_TILE, ROW_TILE)
            now = cur[rows, :]
            before = delayed_tile(cyc, tile, read_slot)
            pieces = []
            for col in range(0, chans, COL_TILE):
                cols = pl.ds(col, COL_TILE)
                f = dot(now, w_sq[cyc, 1, :, cols]) + dot(before, w_sq[cyc, 0, :, cols])
                g = dot(now, w_sq[cyc, 3, :, cols]) + dot(before, w_sq[cyc, 2, :, cols])
                pieces.append((jnp.tanh(f) * (0.5 * jnp.tanh(0.5 * g) + 0.5)).astype(jnp.bfloat16))
            acts.append(jnp.concatenate(pieces, axis=1))
        for tile in range(n_tiles):
            rows = pl.ds(tile * ROW_TILE, ROW_TILE)
            for col in range(0, chans, COL_TILE):
                cols = pl.ds(col, COL_TILE)
                new = h_acc[seq, rows, cols] + dot(acts[tile], w_sq[cyc, 4, :, cols])
                h_acc[seq, rows, cols] = new
                nxt[rows, cols] = new.astype(jnp.bfloat16)
            skip_acc[seq, rows, :] += dot(acts[tile], w_sk[cyc])

    def out_copies(seq, step, remote):
        place = (2 * ((me // 2 + step * 3) % (per_part // 2)) + step // (per_part // 2)) % per_part
        target = part * per_part + place
        rows = pl.ds(place * block_len, block_len)
        which = team * TEAM + seq
        pairs = ((h_acc, h_out, h_send, h_recv), (skip_acc, skip_out, s_send, s_recv))
        if remote:
            return target, [pltpu.make_async_remote_copy(src_ref=acc.at[seq, rows], dst_ref=out.at[which], send_sem=send.at[seq, place],
                                                         recv_sem=recv.at[seq, team], device_id=device(target), device_id_type=MESH)
                            for acc, out, send, recv in pairs]
        return target, [pltpu.make_async_copy(acc.at[seq, rows], out.at[which], recv.at[seq, team]) for acc, out, send, recv in pairs]

    def wait_x(seq, place, _):
        dst = x_buf.at[seq, pl.ds(place * block_len, block_len)]
        pltpu.make_async_copy(dst, dst, x_recv.at[seq, place]).wait()
        return 0

    early = per_part // 2
    lax.fori_loop(0, early, functools.partial(wait_x, 0), 0)
    for seq in range(1, TEAM):
        send_all_x(seq)

    def one_sequence(seq, _):
        lax.fori_loop(jnp.where(seq == 0, early, 0), per_part, functools.partial(wait_x, seq), 0)
        start = x_buf[seq]
        u_buf[0] = start
        h_acc[seq] = start.astype(jnp.float32)
        skip_acc[seq] = jnp.zeros(skip_acc.shape[1:], jnp.float32)

        def one_cycle(rep, _):
            for first in range(0, n_cyc, GROUP):
                stop(seq, rep, first)
                for cyc in range(first, first + GROUP):
                    layer(seq, rep, cyc)
            cycle_end(seq, rep)
            return 0

        lax.fori_loop(0, n_rep, one_cycle, 0)

        def send_out(step, _):
            target, copies = out_copies(seq, step, True)

            @pl.when(target != me)
            def _():
                for copy in copies:
                    copy.start()

            @pl.when(target == me)
            def _():
                for copy in out_copies(seq, step, False)[1]:
                    copy.start()
            return 0

        lax.fori_loop(0, per_part, send_out, 0)
        return 0

    for cyc in range(GROUP):
        for copy in weight_waits(cyc):
            copy.wait()
    lax.fori_loop(0, TEAM, one_sequence, 0)

    @pl.when(part == 0)
    def _():
        for cyc in range(n_cyc - 2 * GROUP + 1, n_cyc):
            halo_copy(0, cyc).wait_send()

    for seq in range(TEAM):
        def finish(step, _, seq=seq):
            to_team, target = x_target(step)

            @pl.when(target != me)
            def _():
                x_copies(seq, to_team, target, True).wait_send()
            target, copies = out_copies(seq, step, True)

            @pl.when(target != me)
            def _():
                for copy in copies:
                    copy.wait_send()
            dst = h_out.at[step * TEAM + seq]
            pltpu.make_async_copy(dst, dst, h_recv.at[seq, step]).wait()
            dst = skip_out.at[step * TEAM + seq]
            pltpu.make_async_copy(dst, dst, s_recv.at[seq, step]).wait()
            return 0

        lax.fori_loop(0, per_part, finish, 0)


def solution(mesh):
    n_hi, n_lo = mesh.shape["seq_hi"], mesh.shape["seq"]
    n_dev = n_hi * n_lo
    seq_spec = P("batch", SEQ_AXES, None)

    def local_stack(x_loc, w_f0, w_f1, w_g0, w_g1, w_res, w_skip):
        n_seq, block_len, chans = x_loc.shape
        n_rep, n_cyc, skip_ch = w_f0.shape[0], w_f0.shape[1], w_skip.shape[-1]
        assert n_seq == n_dev and n_dev % TEAM == 0 and n_cyc % GROUP == 0 and n_cyc % U_BUF == 0
        part_rows = n_dev * block_len // TEAM
        per_part = n_dev // TEAM
        assert part_rows >= 2 ** (n_cyc - 1) and part_rows % ROW_TILE == 0
        halo_rows = halo_layout(n_cyc)[2]
        sem = pltpu.SemaphoreType.DMA
        return pl.pallas_call(
            functools.partial(stack_kernel, n_hi, n_lo, n_rep, n_cyc),
            out_shape=(pltpu.VMEM((n_seq, block_len, chans), jnp.float32), pltpu.VMEM((n_seq, block_len, skip_ch), jnp.float32)),
            in_specs=[pl.BlockSpec(memory_space=pl.ANY)] * 7,
            out_specs=(pl.BlockSpec(memory_space=pltpu.VMEM),) * 2,
            scratch_shapes=[
                pltpu.VMEM((TEAM, part_rows, chans), jnp.bfloat16),
                pltpu.VMEM((TEAM, part_rows, chans), jnp.float32),
                pltpu.VMEM((TEAM, part_rows, skip_ch), jnp.float32),
                pltpu.VMEM((U_BUF, part_rows, chans), jnp.bfloat16),
                pltpu.VMEM((TEAM * n_rep + 1, halo_rows, chans), jnp.bfloat16),
                pltpu.VMEM((n_cyc, 5, chans, chans), jnp.bfloat16),
                pltpu.VMEM((n_cyc, chans, skip_ch), jnp.bfloat16),
                sem((n_cyc, 2)),
                sem((TEAM, per_part)),
                sem((TEAM, per_part)),
                sem((n_cyc,)),
                sem((TEAM * n_rep, n_cyc)),
                sem((TEAM, per_part)),
                sem((TEAM, per_part)),
                sem((TEAM, per_part)),
                sem((TEAM, per_part)),
            ],
            compiler_params=pltpu.CompilerParams(collective_id=0, has_side_effects=True, vmem_limit_bytes=52 * 1024 * 1024),
        )(x_loc, w_f0, w_f1, w_g0, w_g1, w_res, w_skip)

    return jax.shard_map(local_stack, mesh=mesh, in_specs=(seq_spec, P(), P(), P(), P(), P(), P()), out_specs=(seq_spec, seq_spec), check_vma=False)
```
